32 devices in a mesh: gx: 8 (over z, y), yz: 4 (over x, core).
Axes of the slice: x: 2, y: 2, z: 4, core: 2. Of those that a mesh axis runs over, the one named last changes fastest.
Arguments:
- solvent_vel: float32 [3, 256, 128, 2, 128], P(None, 'gx', 'yz'), may hold values from -6 to 6
- occupancy: int32 [256, 128, 128], P('gx', 'yz'), may hold values from 0 to 2
- grid_shift: int32 [3], replicated, may hold values from 1 to 3
- axis_index: int32 [64, 32, 64], P('gx', 'yz'), may hold values from 0 to 63
- colloid_pos: float32 [3, 8, 4, 128], P(None, 'gx', 'yz'), may hold values from 0 to 64, as said below
- colloid_vel: float32 [3, 8, 4, 128], P(None, 'gx', 'yz'), may hold values from -6 to 6
- colloid_mass: float32 [8, 4, 128], P('gx', 'yz'), may hold values from 2 to 20
- colloid_count: int32 [8, 4], P('gx', 'yz'), may hold values from 21 to 128, as said below
Outputs:
- solvent_out: float32 [3, 256, 128, 2, 128], P(None, 'gx', 'yz')
- colloid_pos_out: float32 [3, 8, 4, 128], P(None, 'gx', 'yz')
- colloid_vel_out: float32 [3, 8, 4, 128], P(None, 'gx', 'yz')
The draws below stay inside these ranges and needn't reach their ends.
Inputs may be any that keep to these rules, and one draw needn't show every extreme that they name: `colloid_pos`: component 0 lies in [0, 8), component 1 in [0, 8), component 2 in [0, 64). `colloid_count`: some device holds 128 live colloids in every draw.
All inputs are finite; a program needn't handle non-finite values.
Results may differ from the reference program's by a relative error of at most 0.0003.
Values sent between devices are 32-bit elements; how exact they have to be, the bound alone decides.
A program may use at most 320 MiB of HBM per device.

```python
import math
import jax
import jax.numpy as jnp
from jax import lax

CX = 8
CY = 8
CZ = 64
CMAX = 128
SUB = 4
SLOTS = 2
SUBSTEPS = 4
DIRECTIONS = 64
FX = 32
FY = 32
FZ = 128
NXF = 256
NYF = 128
NX = 64
NY = 32
N_GX = 8
N_YZ = 4


def draw_occupancy(key, part):
    block = 2 * SUB
    blocks_x = (NXF + block - 1) // block
    blocks_y = (NYF + block - 1) // block
    blocks_z = (FZ + 7) // 8
    slots_used = jax.random.randint(jax.random.fold_in(key, 21), (NXF, NYF, FZ), 0, SLOTS + 1)
    sparse = jax.random.randint(jax.random.fold_in(key, 22), (blocks_x * blocks_y * blocks_z,), 0, 4) == 0
    chosen = jax.random.randint(jax.random.fold_in(key, 23), (), 0, blocks_x * blocks_y * blocks_z)
    sparse = jnp.logical_or(sparse, jnp.arange(blocks_x * blocks_y * blocks_z) == chosen)
    sparse = sparse.reshape(blocks_x, blocks_y, blocks_z)
    spread = jnp.repeat(jnp.repeat(jnp.repeat(sparse, block, axis=0), block, axis=1), 8, axis=2)[:NXF, :NYF, :FZ]
    thin_keep = jax.random.randint(jax.random.fold_in(key, 24), (NXF, NYF, FZ), 0, 4) == 0
    keeping = jnp.logical_or(jnp.logical_not(spread), thin_keep)
    return jnp.where(keeping, slots_used, 0).astype(jnp.int32)


def draw_colloid_pos(key, part):
    unit = jax.random.uniform(jax.random.fold_in(key, 5), (3, N_GX, N_YZ, CMAX), jnp.float32)
    extent = jnp.array([CX, CY, CZ], jnp.float32)
    return unit * extent[:, None, None, None] * 0.999


def draw_colloid_count(key, part):
    devices = N_GX * N_YZ
    counts = jax.random.randint(jax.random.fold_in(key, 11), (devices,), CMAX // 6, CMAX // 2 + 1)
    chosen = jax.random.randint(jax.random.fold_in(key, 12), (), 0, devices)
    counts = jnp.where(jnp.arange(devices) == chosen, CMAX, counts)
    return counts.reshape(N_GX, N_YZ).astype(jnp.int32)


def touch_ends(entries, rng, low, high):
    dims = entries.shape
    index_at = [jax.random.randint(jax.random.fold_in(rng, axis), (), 0, dims[axis]) for axis in range(len(dims))]
    entries = entries.at[tuple(index_at)].set(low)
    longest = dims.index(max(dims))
    index_at[longest] = (index_at[longest] + 1) % dims[longest]
    return entries.at[tuple(index_at)].set(high)


def block_levels(key, dims, cuts, low, high):
    def one(dim, parts):
        draws = jax.random.uniform(jax.random.fold_in(jax.random.fold_in(key, 6), dim), (parts,), jnp.float32, low / len(cuts), high / len(cuts))
        return jnp.repeat(jnp.exp(draws), dims[dim] // parts).reshape((-1,) + (1,) * (len(dims) - dim - 1))

    loudness = one(*cuts[0])
    for cut in cuts[1:]:
        loudness = loudness * one(*cut)
    return loudness


def noise(stream_key, dims, scale, bound, split=(), dtype=jnp.bfloat16):
    loudness = block_levels(stream_key, dims, split, -0.22, 0.18) if split else 1.0
    values = jax.random.normal(stream_key, dims, jnp.float32) * scale * loudness
    return jnp.minimum(jnp.maximum(values, -bound), bound).astype(dtype)


def setup_inputs(seed: int = 0) -> dict:
    key_of = jax.random.split(jax.random.key(seed), 9)
    solvent_vel = noise(key_of[0], (3, NXF, NYF, SLOTS, FZ), 1.0, 6.0, ((1, 8), (2, 4)), jnp.float32)
    occupancy = draw_occupancy(jax.random.fold_in(key_of[8], 71), 0)
    grid_shift = jax.random.randint(key_of[2], (3,), 1, SUB).astype(jnp.int32)
    axis_index = touch_ends(jax.random.randint(key_of[3], (NX, NY, CZ), 0, DIRECTIONS), jax.random.fold_in(key_of[3], 1), 0, DIRECTIONS - 1).astype(jnp.int32)
    colloid_pos = draw_colloid_pos(jax.random.fold_in(key_of[8], 71), 0)
    colloid_vel = noise(key_of[5], (3, N_GX, N_YZ, CMAX), 1.0, 6.0, ((1, 8), (2, 4)), jnp.float32)
    colloid_mass = jnp.clip(jnp.exp(math.log(20.0) - 2.3025851 * jax.random.uniform(key_of[6], (N_GX, N_YZ, CMAX), jnp.float32) ** block_levels(key_of[6], (N_GX, N_YZ, CMAX), ((0, 8), (1, 4)), -0.2, 0.2)), 2.0, 20.0)
    colloid_count = draw_colloid_count(jax.random.fold_in(key_of[8], 71), 0)
    return {"solvent_vel": solvent_vel, "occupancy": occupancy, "grid_shift": grid_shift, "axis_index": axis_index, "colloid_pos": colloid_pos, "colloid_vel": colloid_vel, "colloid_mass": colloid_mass, "colloid_count": colloid_count}


turn_angle = 130.0 * math.pi / 180.0
cos_angle = math.cos(turn_angle)
sin_angle = math.sin(turn_angle)
golden = math.pi * (3.0 - math.sqrt(5.0))
cutoff = 1.5
stiffness = 20.0
timestep = 0.05
fill_mass = 16.0

def directions(index):
    number = index.astype(jnp.float32)
    height = 1.0 - (2.0 * number + 1.0) / DIRECTIONS
    radius = jnp.sqrt(1.0 - height * height)
    phase = number * golden
    return jnp.stack([radius * jnp.cos(phase), radius * jnp.sin(phase), height])

def rotate(mean, axis, velocity):
    rel = velocity - mean
    cross = jnp.stack([axis[1] * rel[2] - axis[2] * rel[1], axis[2] * rel[0] - axis[0] * rel[2], axis[0] * rel[1] - axis[1] * rel[0]])
    along = lax.optimization_barrier(jnp.sum(axis * rel, axis=0))
    return mean + cos_angle * rel + sin_angle * cross + (1.0 - cos_angle) * along[None] * axis

def cell_fields(totals, axis_index):
    width_x, width_y, width_z = (totals.shape[1], totals.shape[2], totals.shape[3])
    cells_x, cells_y, cells_z = (width_x // SUB, width_y // SUB, width_z // 2)
    cell = totals.reshape(4, cells_x, SUB, cells_y, SUB, cells_z, 2).sum(axis=(2, 4, 6))
    mean = cell[:3] / jnp.maximum(cell[3], fill_mass)[None]
    both = jnp.concatenate([mean, directions(axis_index)])
    spread = jnp.broadcast_to(both[:, :, None, :, None, :, None], (6, cells_x, SUB, cells_y, SUB, cells_z, 2))
    return spread.reshape(6, width_x, width_y, width_z)

def pair_parts(own, other, other_live):
    diff_x = own[0][..., :, None] - other[0][..., None, :]
    diff_y = own[1][..., :, None] - other[1][..., None, :]
    height = own[2][..., :, None] - other[2][..., None, :]
    height = jnp.where(height > 0.5 * CZ, height - CZ, jnp.where(height < -0.5 * CZ, height + CZ, height))
    radius_sq = diff_x * diff_x + diff_y * diff_y + height * height
    reach = 1.0 - radius_sq / (cutoff * cutoff)
    weight = jnp.where(radius_sq < cutoff * cutoff, reach * reach, 0.0) * other_live[..., None, :]
    return (weight, diff_x, diff_y, height)

def pair_force(own, other, other_live):
    weight, diff_x, diff_y, height = pair_parts(own, other, other_live)
    return stiffness * jnp.stack([lax.optimization_barrier(jnp.sum(weight * diff_x, axis=-1)), lax.optimization_barrier(jnp.sum(weight * diff_y, axis=-1)), lax.optimization_barrier(jnp.sum(weight * height, axis=-1))])

def all_forces(position, alive):
    total = jnp.zeros_like(position)
    for step_x in (-1, 0, 1):
        for step_y in (-1, 0, 1):
            other = jnp.roll(position, (-step_x, -step_y), axis=(1, 2))
            other = jnp.stack([other[0] + step_x * CX, other[1] + step_y * CY, other[2]])
            other_live = jnp.roll(alive, (-step_x, -step_y), axis=(0, 1))
            total = total + pair_force(position, other, other_live)
    return total

def reference(solvent_vel, occupancy, grid_shift, axis_index, colloid_pos, colloid_vel, colloid_mass, colloid_count):
    nxf, nyf, nzf = occupancy.shape
    live = (lax.broadcasted_iota(jnp.int32, solvent_vel.shape[1:], 2) < occupancy[:, :, None, :]).astype(jnp.float32)
    moment = solvent_vel * live[None]
    alive = (lax.broadcasted_iota(jnp.int32, colloid_mass.shape, 2) < colloid_count[:, :, None]).astype(jnp.float32)
    row = lax.broadcasted_iota(jnp.int32, colloid_mass.shape, 0)
    column = lax.broadcasted_iota(jnp.int32, colloid_mass.shape, 1)
    cell_x = row * FX + jnp.clip(jnp.floor(colloid_pos[0] * SUB).astype(jnp.int32), 0, FX - 1)
    cell_y = column * FY + jnp.clip(jnp.floor(colloid_pos[1] * SUB).astype(jnp.int32), 0, FY - 1)
    cell_z = jnp.clip(jnp.floor(colloid_pos[2] * 2.0).astype(jnp.int32), 0, FZ - 1)
    flat = ((cell_x * nyf + cell_y) * nzf + cell_z).reshape(-1)
    weight = colloid_mass * alive
    values = jnp.concatenate([colloid_vel * weight[None], weight[None]]).reshape(4, -1)
    deposit = jnp.zeros((4, nxf * nyf * nzf), jnp.float32).at[:, flat].add(values).reshape(4, nxf, nyf, nzf)
    totals = jnp.concatenate([lax.optimization_barrier(jnp.sum(moment, axis=3)), lax.optimization_barrier(jnp.sum(live, axis=2))[None]]) + deposit
    forward = (grid_shift[0], grid_shift[1], grid_shift[2])
    backward = (-grid_shift[0], -grid_shift[1], -grid_shift[2])
    totals = jnp.roll(totals, forward, axis=(1, 2, 3))
    fields = jnp.roll(cell_fields(totals, axis_index), backward, axis=(1, 2, 3))
    turned = rotate(fields[:3, :, :, None], fields[3:, :, :, None], solvent_vel)
    solvent_out = jnp.where(live[None] > 0, turned, solvent_vel)
    picked = fields.reshape(6, -1)[:, flat].reshape((6,) + colloid_mass.shape)
    velocity = jnp.where(alive[None] > 0, rotate(picked[:3], picked[3:], colloid_vel), colloid_vel)
    position = colloid_pos
    for step in range(SUBSTEPS):
        force = all_forces(position, alive)
        velocity = velocity + timestep * force / colloid_mass[None]
        position = position + timestep * velocity
    keep = alive[None] > 0
    return (solvent_out, jnp.where(keep, position, colloid_pos), jnp.where(keep, velocity, colloid_vel))
```

```python
import functools
import math

import jax
import jax.numpy as jnp
from jax import lax
from jax.experimental import pallas as pl
from jax.experimental.pallas import tpu as pltpu
from jax.sharding import PartitionSpec as P

CX = 8
CY = 8
CZ = 64
SUB = 4
SUBSTEPS = 4
DIRECTIONS = 64


turn_angle = 130.0 * math.pi / 180.0
cos_angle = math.cos(turn_angle)
sin_angle = math.sin(turn_angle)
golden = math.pi * (3.0 - math.sqrt(5.0))
cutoff = 1.5
stiffness = 20.0
timestep = 0.05
fill_mass = 16.0
MESH = pl.DeviceIdType.MESH


def iota(shape, dim):
    return lax.broadcasted_iota(jnp.int32, shape, dim)


def three_terms(value):
    high = value.astype(jnp.bfloat16)
    rest = value - high.astype(jnp.float32)
    middle = rest.astype(jnp.bfloat16)
    low = (rest - middle.astype(jnp.float32)).astype(jnp.bfloat16)
    return (high, middle, low)


def dot(left, right, contract=((1,), (0,))):
    return lax.dot_general(left, right, (contract, ((), ())), preferred_element_type=jnp.float32)


def wrapped(value, size):
    return jnp.where(value >= size, value - size, value)


def layer_of(row, scale, width):
    return jnp.clip(jnp.floor(row * scale).astype(jnp.int32), 0, width - 1)


def sums_kernel(shape, steps, shift, count, solvent, occupancy, pos, vel, mass, out, acc):
    width_x, width_y, width_z = shape
    cells_x, cells_y = (width_x // SUB + 1, width_y // SUB + 1)
    block_x = width_x // steps
    rows = 2 * width_y
    step = pl.program_id(0)
    shift_x, shift_y, shift_z = (shift[0], shift[1], shift[2])

    @pl.when(step == 0)
    def _():
        acc[...] = jnp.zeros_like(acc)

    double = (iota((rows, width_y), 0) >> 1 == iota((rows, width_y), 1)).astype(jnp.bfloat16)
    slot = (iota((rows, width_z), 0) & 1).astype(jnp.float32)
    for x in range(block_x):
        filled = occupancy[x].astype(jnp.float32)
        live = dot(double, filled.astype(jnp.bfloat16)) > slot
        cell = (step * block_x + x + shift_x) >> 2
        for c in range(3):
            at = pl.ds(c * rows, rows)
            acc[cell, at, :] += jnp.where(live, solvent[c, x], 0.0)
        acc[cell, pl.ds(3 * rows, width_y), :] += filled

    @pl.when(step == steps - 1)
    def _():
        total = 3 * rows + width_y
        column = iota((cells_y * 8, total), 1)
        target = iota((cells_y * 8, total), 0)
        heavy = column >= 3 * rows
        part = jnp.where(heavy, 3, (column >= rows).astype(jnp.int32) + (column >= 2 * rows).astype(jnp.int32))
        layer = jnp.where(heavy, column - 3 * rows, (column - part * rows) >> 1)
        fits = jnp.logical_and(part == (target & 7), ((layer + shift_y) >> 2) == (target >> 3))
        select = fits.astype(jnp.float32).astype(jnp.bfloat16)

        cell_x = (layer_of(pos[0, 0], SUB, width_x) + shift_x) >> 2
        cell_y = (layer_of(pos[1, 0], SUB, width_y) + shift_y) >> 2
        cell_z = wrapped(layer_of(pos[2, 0], 2.0, width_z) + shift_z, width_z) >> 1
        slots = mass.shape[2]
        alive = (iota((1, slots), 1) < count[0, 0]).astype(jnp.float32)
        weight = mass[0] * alive
        comp = iota((8, slots), 0)
        values = jnp.where(
            comp == 0,
            vel[0, 0] * weight,
            jnp.where(
                comp == 1,
                vel[1, 0] * weight,
                jnp.where(comp == 2, vel[2, 0] * weight, jnp.where(comp == 3, weight, 0.0)),
            ),
        )
        place = jnp.broadcast_to(cell_x * cells_y + cell_y, (8, slots))
        near = (wrapped(iota((width_z, slots), 0) + shift_z, width_z) >> 1) == cell_z
        near = near.astype(jnp.float32).astype(jnp.bfloat16)
        even = ((iota((cells_y * 8, width_z), 1) + shift_z) & 1) == 0
        for i in range(cells_x):
            sums = sum(dot(select, term) for term in three_terms(acc[i])[::-1])
            partner = jnp.where(
                even, pltpu.roll(sums, width_z - 1, 1), pltpu.roll(sums, 1, 1)
            )
            number = iota((cells_y, 8, slots), 0) + i * cells_y
            spread = jnp.where(number == place[None], values[None], 0.0).reshape(cells_y * 8, slots)
            deposit = sum(dot(term, near, ((1,), (1,))) for term in three_terms(spread)[::-1])
            out[i] = (sums + partner + deposit).reshape(cells_y, 8, width_z)


def exchange_kernel(
    shape, shift, count, part, axis, pos, vel, mass, fields, pos_out, vel_out,
    halo_x, halo_y, halo_c, edge_x, edge_y, edge_c, sent, got, own, force,
    halo_sem, edge_sem, sent_sem, got_sem,
):
    width_x, width_y, width_z = shape
    n_x, n_y = (width_x // SUB, width_y // SUB)
    slots = mass.shape[2]
    me_x, me_y = (lax.axis_index("gx"), lax.axis_index("yz"))
    size_x, size_y = (lax.axis_size("gx"), lax.axis_size("yz"))
    shift_x, shift_y, shift_z = (shift[0], shift[1], shift[2])

    def device(a, b):
        return (lax.rem(me_x + a + size_x, size_x), lax.rem(me_y + b + size_y, size_y))

    around = [(a, b) for a in (-1, 0, 1) for b in (-1, 0, 1) if (a, b) != (0, 0)]
    barrier = pltpu.get_barrier_semaphore()
    for a, b in around:
        pl.semaphore_signal(barrier, inc=1, device_id=device(a, b), device_id_type=MESH)

    alive = (iota((1, slots), 1) < count[0, 0]).astype(jnp.float32)
    comp = iota((8, slots), 0)

    def stacked(rows):
        out = jnp.zeros((8, slots), jnp.float32)
        for c, row in enumerate(rows):
            out = jnp.where(comp == c, row, out)
        return out

    def columns(rows):
        block = jnp.concatenate([rows, jnp.zeros((slots - 8, slots), jnp.float32)], axis=0)
        return block.T

    start_rows = stacked([pos[0, 0], pos[1, 0], pos[2, 0], alive, mass[0]])
    sent[0] = start_rows
    pl.semaphore_wait(barrier, len(around))

    def remote(src, dst, send, receive, where):
        return pltpu.make_async_remote_copy(
            src_ref=src, dst_ref=dst, send_sem=send, recv_sem=receive,
            device_id=where, device_id_type=MESH,
        )

    halo = [
        remote(part.at[n_x, pl.ds(0, n_y)], halo_x, halo_sem.at[0], halo_sem.at[3], device(1, 0)),
        remote(part.at[pl.ds(0, n_x), n_y], halo_y, halo_sem.at[1], halo_sem.at[4], device(0, 1)),
        remote(part.at[n_x, n_y], halo_c, halo_sem.at[2], halo_sem.at[5], device(1, 1)),
    ]
    for copy in halo:
        copy.start()

    def exchange(step):
        copies = []
        for k, (a, b) in enumerate(around):
            copies.append(
                remote(
                    sent.at[step], got.at[step, 7 - k],
                    sent_sem.at[step, k], got_sem.at[step, 7 - k], device(a, b),
                )
            )
        for copy in copies:
            copy.start()
        return copies

    copies = exchange(0)

    state = columns(start_rows)
    place = [state[:, c : c + 1] for c in range(3)]
    mass_column = state[:, 4:5]

    index = axis[...].reshape(n_x * n_y, width_z // 2).astype(jnp.float32).astype(jnp.bfloat16)
    cell_z = wrapped(iota((width_z // 2, width_z), 1) + shift_z, width_z) >> 1
    expand = (cell_z == iota((width_z // 2, width_z), 0)).astype(jnp.float32).astype(jnp.bfloat16)
    number = dot(index, expand)
    height = 1.0 - (2.0 * number + 1.0) / DIRECTIONS
    radius = jnp.sqrt(1.0 - height * height)
    phase = number * golden
    normal = [radius * jnp.cos(phase), radius * jnp.sin(phase), height]
    sub = iota((n_x * n_y, 8, width_z), 1)
    spread = [jnp.broadcast_to(n[:, None, :], (n_x * n_y, 8, width_z)) for n in normal]
    directions = jnp.where(sub == 3, spread[0], jnp.where(sub == 4, spread[1], spread[2]))
    fields[pl.ds(0, n_x), pl.ds(0, n_y)] = directions.reshape(n_x, n_y, 8, width_z)

    for copy in halo:
        copy.wait()
    sub = iota((n_y, 8, width_z), 1)
    for i in range(n_x):
        total = part[i, pl.ds(0, n_y)]
        first = halo_y[i][None]
        if i == 0:
            total = total + halo_x[...]
            first = first + halo_c[...][None]
        total = jnp.concatenate([total[:1] + first, total[1:]], axis=0)
        mean = total / jnp.maximum(total[:, 3:4, :], fill_mass)
        fields[i, pl.ds(0, n_y)] = jnp.where(sub < 3, mean, fields[i, pl.ds(0, n_y)])
    edges = [
        remote(fields.at[0, pl.ds(0, n_y)], edge_x, edge_sem.at[0], edge_sem.at[3], device(-1, 0)),
        remote(fields.at[pl.ds(0, n_x), 0], edge_y, edge_sem.at[1], edge_sem.at[4], device(0, -1)),
        remote(fields.at[0, 0], edge_c, edge_sem.at[2], edge_sem.at[5], device(-1, -1)),
    ]
    for copy in edges:
        copy.start()

    def forces(step, copies, place):
        for c in range(3):
            own[c] = jnp.broadcast_to(place[c], (slots, slots))
        for copy in copies:
            copy.wait()

        def block(r, carry):
            at = pl.ds(pl.multiple_of(r * 8, 8), 8)
            own_x, own_y, own_z = (own[0, at, :], own[1, at, :], own[2, at, :])
            total = [jnp.zeros((8, slots), jnp.float32)] * 3
            sources = [((0, 0), None)] + [(pair, k) for k, pair in enumerate(around)]
            for (a, b), k in sources:
                def row(c):
                    if k is None:
                        return sent[step, pl.ds(c, 1), :]
                    return got[step, k, pl.ds(c, 1), :]

                diff_x = own_x - (row(0) + float(a * CX))
                diff_y = own_y - (row(1) + float(b * CY))
                high = own_z - row(2)
                high = jnp.where(
                    high > 0.5 * CZ, high - CZ, jnp.where(high < -0.5 * CZ, high + CZ, high)
                )
                radius_sq = diff_x * diff_x + diff_y * diff_y + high * high
                reach = 1.0 - radius_sq * (1.0 / (cutoff * cutoff))
                weight = jnp.where(radius_sq < cutoff * cutoff, reach * reach, 0.0) * row(3)
                total = [
                    total[0] + weight * diff_x,
                    total[1] + weight * diff_y,
                    total[2] + weight * high,
                ]
            for c in range(3):
                force[c, at, :] = total[c]
            return carry

        lax.fori_loop(0, slots // 8, block, 0)
        return [stiffness * jnp.sum(force[c], axis=1, keepdims=True) for c in range(3)]

    push = forces(0, copies, place)

    for copy in edges:
        copy.wait()
    fields[n_x, pl.ds(0, n_y)] = edge_x[...]
    fields[pl.ds(0, n_x), n_y] = edge_y[...]
    fields[n_x, n_y] = edge_c[...]

    layer_z = layer_of(pos[2, 0], 2.0, width_z)
    cell_x = (layer_of(pos[0, 0], SUB, width_x) + shift_x) >> 2
    cell_y = (layer_of(pos[1, 0], SUB, width_y) + shift_y) >> 2
    target = jnp.broadcast_to(cell_x * (n_y + 1) + cell_y, (8, slots))
    chosen = (iota((width_z, slots), 0) == layer_z).astype(jnp.float32).astype(jnp.bfloat16)
    picked = jnp.zeros((8, slots), jnp.float32)
    for i in range(n_x + 1):
        rows = fields[i].reshape((n_y + 1) * 8, width_z)
        at_z = sum(dot(term, chosen) for term in three_terms(rows)[::-1])
        number = iota((n_y + 1, 8, slots), 0) + i * (n_y + 1)
        at_z = at_z.reshape(n_y + 1, 8, slots)
        picked = picked + jnp.sum(jnp.where(number == target[None], at_z, 0.0), axis=0)
    mean = [picked[c : c + 1] for c in range(3)]
    n = [picked[c : c + 1] for c in range(3, 6)]
    rel = [vel[c, 0] - mean[c] for c in range(3)]
    cross = [n[1] * rel[2] - n[2] * rel[1], n[2] * rel[0] - n[0] * rel[2], n[0] * rel[1] - n[1] * rel[0]]
    along = n[0] * rel[0] + n[1] * rel[1] + n[2] * rel[2]
    turned = [
        mean[c] + cos_angle * rel[c] + sin_angle * cross[c] + (1.0 - cos_angle) * along * n[c]
        for c in range(3)
    ]
    state = columns(stacked([jnp.where(alive > 0, turned[c], vel[c, 0]) for c in range(3)]))
    speed = [state[:, c : c + 1] for c in range(3)]

    lane = iota((slots, slots), 1)
    for step in range(SUBSTEPS):
        speed = [speed[c] + timestep * push[c] / mass_column for c in range(3)]
        place = [place[c] + timestep * speed[c] for c in range(3)]
        block = jnp.zeros((slots, slots), jnp.float32)
        for c, column in enumerate(place):
            block = jnp.where(lane == c, column, block)
        if step == SUBSTEPS - 1:
            for c, column in enumerate(speed):
                block = jnp.where(lane == 3 + c, column, block)
        flipped = block.T[:8]
        if step < SUBSTEPS - 1:
            sent[step + 1] = jnp.where(comp == 3, alive, flipped)
            copies = exchange(step + 1)
            push = forces(step + 1, copies, place)
    for c in range(3):
        pos_out[c, 0] = jnp.where(alive > 0, flipped[c : c + 1], pos[c, 0])
        vel_out[c, 0] = jnp.where(alive > 0, flipped[3 + c : 4 + c], vel[c, 0])


def rotate_kernel(shape, steps, shift, solvent, occupancy, fields, out):
    width_x, width_y, width_z = shape
    block_x = width_x // steps
    n_y = width_y // SUB
    rows = 2 * width_y
    step = pl.program_id(0)
    shift_x, shift_y = (shift[0], shift[1])
    double = (iota((rows, width_y), 0) >> 1 == iota((rows, width_y), 1)).astype(jnp.bfloat16)
    row = iota((8, width_z), 0)
    slot = (row & 1).astype(jnp.float32)
    later = ((row >> 1) + shift_y) >= SUB

    def layer(x, carry):
        held = dot(double, occupancy[x].astype(jnp.float32).astype(jnp.bfloat16))
        cell = (step * block_x + x + shift_x) >> 2
        for b in range(n_y):
            at = pl.ds(8 * b, 8)
            both = [
                jnp.where(
                    later, fields[cell, b + 1, pl.ds(c, 1), :], fields[cell, b, pl.ds(c, 1), :]
                )
                for c in range(6)
            ]
            mean, n = (both[:3], both[3:])
            old = [solvent[c, x, at, :] for c in range(3)]
            rel = [old[c] - mean[c] for c in range(3)]
            along = (1.0 - cos_angle) * (n[0] * rel[0] + n[1] * rel[1] + n[2] * rel[2])
            cross = [
                n[1] * rel[2] - n[2] * rel[1],
                n[2] * rel[0] - n[0] * rel[2],
                n[0] * rel[1] - n[1] * rel[0],
            ]
            live = held[8 * b : 8 * b + 8] > slot
            for c in range(3):
                new = mean[c] + cos_angle * rel[c] + sin_angle * cross[c] + along * n[c]
                out[c, x, at, :] = jnp.where(live, new, old[c])
        return carry

    lax.fori_loop(0, block_x, layer, 0)


def per_device(
    solvent_vel,
    occupancy,
    grid_shift,
    axis_index,
    colloid_pos,
    colloid_vel,
    colloid_mass,
    colloid_count,
):
    shape = occupancy.shape
    width_x, width_y, width_z = shape
    rows = 2 * width_y
    n_x, n_y = (width_x // SUB, width_y // SUB)
    slots = colloid_mass.shape[2]
    steps = 4
    block_x = width_x // steps
    solvent = solvent_vel.reshape(3, width_x, rows, width_z)
    smem = pl.BlockSpec(memory_space=pltpu.SMEM)
    vmem = pl.BlockSpec(memory_space=pltpu.VMEM)
    solvent_spec = pl.BlockSpec((3, block_x, rows, width_z), lambda i: (0, i, 0, 0))
    occupancy_spec = pl.BlockSpec((block_x, width_y, width_z), lambda i: (i, 0, 0))
    cells = (n_x + 1, n_y + 1, 8, width_z)
    f32 = jnp.float32

    part = pl.pallas_call(
        functools.partial(sums_kernel, shape, steps),
        out_shape=jax.ShapeDtypeStruct(cells, f32),
        grid=(steps,),
        in_specs=[smem, smem, solvent_spec, occupancy_spec, vmem, vmem, vmem],
        out_specs=vmem,
        scratch_shapes=[pltpu.VMEM((n_x + 1, 3 * rows + width_y, width_z), f32)],
        name="sums",
    )(grid_shift, colloid_count, solvent, occupancy, colloid_pos, colloid_vel, colloid_mass)

    fields, pos_out, vel_out = pl.pallas_call(
        functools.partial(exchange_kernel, shape),
        out_shape=[
            jax.ShapeDtypeStruct(cells, f32),
            jax.ShapeDtypeStruct(colloid_pos.shape, f32),
            jax.ShapeDtypeStruct(colloid_vel.shape, f32),
        ],
        in_specs=[smem, smem] + [vmem] * 5,
        out_specs=[vmem] * 3,
        scratch_shapes=[
            pltpu.VMEM((n_y, 8, width_z), f32),
            pltpu.VMEM((n_x, 8, width_z), f32),
            pltpu.VMEM((8, width_z), f32),
            pltpu.VMEM((n_y, 8, width_z), f32),
            pltpu.VMEM((n_x, 8, width_z), f32),
            pltpu.VMEM((8, width_z), f32),
            pltpu.VMEM((SUBSTEPS, 8, slots), f32),
            pltpu.VMEM((SUBSTEPS, 8, 8, slots), f32),
            pltpu.VMEM((3, slots, slots), f32),
            pltpu.VMEM((3, slots, slots), f32),
            pltpu.SemaphoreType.DMA((6,)),
            pltpu.SemaphoreType.DMA((6,)),
            pltpu.SemaphoreType.DMA((SUBSTEPS, 8)),
            pltpu.SemaphoreType.DMA((SUBSTEPS, 8)),
        ],
        compiler_params=pltpu.CompilerParams(collective_id=0, has_side_effects=True),
        name="exchange",
    )(grid_shift, colloid_count, part, axis_index, colloid_pos, colloid_vel, colloid_mass)

    solvent_out = pl.pallas_call(
        functools.partial(rotate_kernel, shape, steps),
        out_shape=jax.ShapeDtypeStruct(solvent.shape, f32),
        grid=(steps,),
        in_specs=[smem, solvent_spec, occupancy_spec, vmem],
        out_specs=solvent_spec,
        name="rotate",
    )(grid_shift, solvent, occupancy, fields)
    return (solvent_out.reshape(solvent_vel.shape), pos_out, vel_out)


def solution(mesh):
    return jax.shard_map(
        per_device,
        mesh=mesh,
        in_specs=(
            P(None, "gx", "yz", None, None),
            P("gx", "yz", None),
            P(),
            P("gx", "yz", None),
            P(None, "gx", "yz", None),
            P(None, "gx", "yz", None),
            P("gx", "yz", None),
            P("gx", "yz"),
        ),
        out_specs=(
            P(None, "gx", "yz", None, None),
            P(None, "gx", "yz", None),
            P(None, "gx", "yz", None),
        ),
        check_vma=False,
    )
```

```python
import functools
import math

import jax
import jax.numpy as jnp
from jax import lax
from jax.experimental import pallas as pl
from jax.experimental.pallas import tpu as pltpu
from jax.sharding import PartitionSpec as P

CX = 8
CY = 8
CZ = 64
SUB = 4
SUBSTEPS = 4
DIRECTIONS = 64


turn_angle = 130.0 * math.pi / 180.0
cos_angle = math.cos(turn_angle)
sin_angle = math.sin(turn_angle)
golden = math.pi * (3.0 - math.sqrt(5.0))
cutoff = 1.5
stiffness = 20.0
timestep = 0.05
fill_mass = 16.0
MESH = pl.DeviceIdType.MESH


def iota(shape, dim):
    return lax.broadcasted_iota(jnp.int32, shape, dim)


def three_terms(value):
    high = value.astype(jnp.bfloat16)
    rest = value - high.astype(jnp.float32)
    middle = rest.astype(jnp.bfloat16)
    low = (rest - middle.astype(jnp.float32)).astype(jnp.bfloat16)
    return (high, middle, low)


def dot(left, right, contract=((1,), (0,))):
    return lax.dot_general(left, right, (contract, ((), ())), preferred_element_type=jnp.float32)


def wrapped(value, size):
    return jnp.where(value >= size, value - size, value)


def layer_of(row, scale, width):
    return jnp.clip(jnp.floor(row * scale).astype(jnp.int32), 0, width - 1)


def accumulate(shape, steps, shift_x, solvent, occupancy, acc):
    width_x, width_y, width_z = shape
    block_x = width_x // steps
    rows = 2 * width_y
    step = pl.program_id(0)

    @pl.when(step == 0)
    def _():
        acc[...] = jnp.zeros_like(acc)

    double = (iota((rows, width_y), 0) >> 1 == iota((rows, width_y), 1)).astype(jnp.bfloat16)
    slot = (iota((rows, width_z), 0) & 1).astype(jnp.float32)
    for first in range(0, block_x, SUB):
        cell = step * (block_x // SUB) + first // SUB
        filled = [occupancy[first + r].astype(jnp.float32) for r in range(SUB)]
        live = [dot(double, f.astype(jnp.bfloat16)) > slot for f in filled]
        for c in range(4):
            size = rows if c < 3 else width_y
            at = pl.ds(c * rows, size)
            near = jnp.zeros((size, width_z), jnp.float32)
            far = near
            for r in range(SUB):
                value = jnp.where(live[r], solvent[c, first + r], 0.0) if c < 3 else filled[r]
                stays = jnp.broadcast_to(shift_x + r, (size, width_z)) < SUB
                near = near + jnp.where(stays, value, 0.0)
                far = far + jnp.where(stays, 0.0, value)
            acc[cell, at, :] += near
            acc[cell + 1, at, :] += far


def cell_sums(shape, shift, count, pos, vel, mass, part, acc):
    width_x, width_y, width_z = shape
    cells_x, cells_y = (width_x // SUB + 1, width_y // SUB + 1)
    rows = 2 * width_y
    shift_x, shift_y, shift_z = (shift[0], shift[1], shift[2])
    total = 3 * rows + width_y
    column = iota((cells_y * 8, total), 1)
    target = iota((cells_y * 8, total), 0)
    heavy = column >= 3 * rows
    which = jnp.where(heavy, 3, (column >= rows).astype(jnp.int32) + (column >= 2 * rows).astype(jnp.int32))
    layer = jnp.where(heavy, column - 3 * rows, (column - which * rows) >> 1)
    fits = jnp.logical_and(which == (target & 7), ((layer + shift_y) >> 2) == (target >> 3))
    select = fits.astype(jnp.float32).astype(jnp.bfloat16)

    cell_x = (layer_of(pos[0, 0], SUB, width_x) + shift_x) >> 2
    cell_y = (layer_of(pos[1, 0], SUB, width_y) + shift_y) >> 2
    cell_z = wrapped(layer_of(pos[2, 0], 2.0, width_z) + shift_z, width_z) >> 1
    slots = mass.shape[2]
    alive = (iota((1, slots), 1) < count[0, 0]).astype(jnp.float32)
    weight = mass[0] * alive
    comp = iota((8, slots), 0)
    values = jnp.where(
        comp == 0,
        vel[0, 0] * weight,
        jnp.where(
            comp == 1,
            vel[1, 0] * weight,
            jnp.where(comp == 2, vel[2, 0] * weight, jnp.where(comp == 3, weight, 0.0)),
        ),
    )
    place = jnp.broadcast_to(cell_x * cells_y + cell_y, (8, slots))
    near = (wrapped(iota((width_z, slots), 0) + shift_z, width_z) >> 1) == cell_z
    near = near.astype(jnp.float32).astype(jnp.bfloat16)
    even = ((iota((cells_y * 8, width_z), 1) + shift_z) & 1) == 0
    for i in range(cells_x):
        sums = sum(dot(select, term) for term in three_terms(acc[i])[::-1])
        partner = jnp.where(
            even, pltpu.roll(sums, width_z - 1, 1), pltpu.roll(sums, 1, 1)
        )
        number = iota((cells_y, 8, slots), 0) + i * cells_y
        spread = jnp.where(number == place[None], values[None], 0.0).reshape(cells_y * 8, slots)
        deposit = sum(dot(term, near, ((1,), (1,))) for term in three_terms(spread)[::-1])
        part[i] = (sums + partner + deposit).reshape(cells_y, 8, width_z)


def exchange_kernel(
    shape, steps, shift, count, solvent, occupancy, axis, pos, vel, mass, fields, pos_out, vel_out,
    acc, part, halo_x, halo_y, halo_c, edge_x, edge_y, edge_c, sent, got, own, force,
    halo_sem, edge_sem, sent_sem, got_sem,
):
    width_x, width_y, width_z = shape
    n_x, n_y = (width_x // SUB, width_y // SUB)
    slots = mass.shape[2]
    me_x, me_y = (lax.axis_index("gx"), lax.axis_index("yz"))
    size_x, size_y = (lax.axis_size("gx"), lax.axis_size("yz"))
    shift_x, shift_y, shift_z = (shift[0], shift[1], shift[2])

    def device(a, b):
        return (lax.rem(me_x + a + size_x, size_x), lax.rem(me_y + b + size_y, size_y))

    around = [(a, b) for a in (-1, 0, 1) for b in (-1, 0, 1) if (a, b) != (0, 0)]
    barrier = pltpu.get_barrier_semaphore()
    grid_step = pl.program_id(0)

    @pl.when(grid_step == 0)
    def _():
        for a, b in around:
            pl.semaphore_signal(barrier, inc=1, device_id=device(a, b), device_id_type=MESH)

    accumulate(shape, steps, shift_x, solvent, occupancy, acc)

    @pl.when(grid_step == steps - 1)
    def _():
        alive = (iota((1, slots), 1) < count[0, 0]).astype(jnp.float32)
        comp = iota((8, slots), 0)

        def stacked(rows):
            out = jnp.zeros((8, slots), jnp.float32)
            for c, row in enumerate(rows):
                out = jnp.where(comp == c, row, out)
            return out

        def columns(rows):
            block = jnp.concatenate([rows, jnp.zeros((slots - 8, slots), jnp.float32)], axis=0)
            return block.T

        start_rows = stacked([pos[0, 0], pos[1, 0], pos[2, 0], alive, mass[0]])
        sent[0] = start_rows
        pl.semaphore_wait(barrier, len(around))

        def remote(src, dst, send, receive, where):
            return pltpu.make_async_remote_copy(
                src_ref=src, dst_ref=dst, send_sem=send, recv_sem=receive,
                device_id=where, device_id_type=MESH,
            )

        def exchange(step):
            copies = []
            for k, (a, b) in enumerate(around):
                copies.append(
                    remote(
                        sent.at[step], got.at[step, 7 - k],
                        sent_sem.at[step, k], got_sem.at[step, 7 - k], device(a, b),
                    )
                )
            for copy in copies:
                copy.start()
            return copies

        copies = exchange(0)

        cell_sums(shape, shift, count, pos, vel, mass, part, acc)
        halo = [
            remote(part.at[n_x, pl.ds(0, n_y)], halo_x, halo_sem.at[0], halo_sem.at[3], device(1, 0)),
            remote(part.at[pl.ds(0, n_x), n_y], halo_y, halo_sem.at[1], halo_sem.at[4], device(0, 1)),
            remote(part.at[n_x, n_y], halo_c, halo_sem.at[2], halo_sem.at[5], device(1, 1)),
        ]
        for copy in halo:
            copy.start()

        state = columns(start_rows)
        place = [state[:, c : c + 1] for c in range(3)]
        mass_column = state[:, 4:5]

        index = axis[...].reshape(n_x * n_y, width_z // 2).astype(jnp.float32).astype(jnp.bfloat16)
        cell_z = wrapped(iota((width_z // 2, width_z), 1) + shift_z, width_z) >> 1
        expand = (cell_z == iota((width_z // 2, width_z), 0)).astype(jnp.float32).astype(jnp.bfloat16)
        number = dot(index, expand)
        height = 1.0 - (2.0 * number + 1.0) / DIRECTIONS
        radius = jnp.sqrt(1.0 - height * height)
        phase = number * golden
        normal = [radius * jnp.cos(phase), radius * jnp.sin(phase), height]
        sub = iota((n_x * n_y, 8, width_z), 1)
        spread = [jnp.broadcast_to(n[:, None, :], (n_x * n_y, 8, width_z)) for n in normal]
        directions = jnp.where(sub == 3, spread[0], jnp.where(sub == 4, spread[1], spread[2]))
        fields[pl.ds(0, n_x), pl.ds(0, n_y)] = directions.reshape(n_x, n_y, 8, width_z)

        for copy in halo:
            copy.wait()
        sub = iota((n_y, 8, width_z), 1)
        for i in range(n_x):
            total = part[i, pl.ds(0, n_y)]
            first = halo_y[i][None]
            if i == 0:
                total = total + halo_x[...]
                first = first + halo_c[...][None]
            total = jnp.concatenate([total[:1] + first, total[1:]], axis=0)
            mean = total / jnp.maximum(total[:, 3:4, :], fill_mass)
            fields[i, pl.ds(0, n_y)] = jnp.where(sub < 3, mean, fields[i, pl.ds(0, n_y)])
        edges = [
            remote(fields.at[0, pl.ds(0, n_y)], edge_x, edge_sem.at[0], edge_sem.at[3], device(-1, 0)),
            remote(fields.at[pl.ds(0, n_x), 0], edge_y, edge_sem.at[1], edge_sem.at[4], device(0, -1)),
            remote(fields.at[0, 0], edge_c, edge_sem.at[2], edge_sem.at[5], device(-1, -1)),
        ]
        for copy in edges:
            copy.start()

        groups = [
            [(pair, k) for k, pair in enumerate(around) if 0 in pair],
            [(pair, k) for k, pair in enumerate(around) if 0 not in pair],
        ]
        wide = 32 if slots % 32 == 0 else 8

        def forces(step, copies, place):
            for c in range(3):
                own[c] = jnp.broadcast_to(place[c], (slots, slots))

            for sources in [[((0, 0), None)]] + groups:
                for _, k in sources:
                    if k is not None:
                        copies[7 - k].wait_recv()

                def block(r, carry, sources=sources):
                    at = pl.ds(pl.multiple_of(r * wide, 8), wide)
                    own_x, own_y, own_z = (own[0, at, :], own[1, at, :], own[2, at, :])
                    total = None
                    for (a, b), k in sources:
                        def row(c):
                            if k is None:
                                return sent[step, pl.ds(c, 1), :]
                            return got[step, k, pl.ds(c, 1), :]

                        diff_x = own_x - (row(0) + float(a * CX))
                        diff_y = own_y - (row(1) + float(b * CY))
                        high = own_z - row(2)
                        high = jnp.where(
                            high > 0.5 * CZ, high - CZ, jnp.where(high < -0.5 * CZ, high + CZ, high)
                        )
                        radius_sq = diff_x * diff_x + diff_y * diff_y + high * high
                        reach = 1.0 - radius_sq * (1.0 / (cutoff * cutoff))
                        weight = jnp.where(radius_sq < cutoff * cutoff, reach * reach, 0.0) * row(3)
                        parts = [weight * diff_x, weight * diff_y, weight * high]
                        total = parts if total is None else [total[c] + parts[c] for c in range(3)]
                    for c in range(3):
                        if sources[0][1] is None:
                            force[c, at, :] = total[c]
                        else:
                            force[c, at, :] += total[c]
                    return carry

                lax.fori_loop(0, slots // wide, block, 0)
            for copy in copies:
                copy.wait_send()
            return [stiffness * jnp.sum(force[c], axis=1, keepdims=True) for c in range(3)]

        push = forces(0, copies, place)

        for copy in edges:
            copy.wait()
        fields[n_x, pl.ds(0, n_y)] = edge_x[...]
        fields[pl.ds(0, n_x), n_y] = edge_y[...]
        fields[n_x, n_y] = edge_c[...]

        layer_z = layer_of(pos[2, 0], 2.0, width_z)
        cell_x = (layer_of(pos[0, 0], SUB, width_x) + shift_x) >> 2
        cell_y = (layer_of(pos[1, 0], SUB, width_y) + shift_y) >> 2
        target = jnp.broadcast_to(cell_x * (n_y + 1) + cell_y, (8, slots))
        chosen = (iota((width_z, slots), 0) == layer_z).astype(jnp.float32).astype(jnp.bfloat16)
        picked = jnp.zeros((8, slots), jnp.float32)
        for i in range(n_x + 1):
            rows = fields[i].reshape((n_y + 1) * 8, width_z)
            at_z = sum(dot(term, chosen) for term in three_terms(rows)[::-1])
            number = iota((n_y + 1, 8, slots), 0) + i * (n_y + 1)
            at_z = at_z.reshape(n_y + 1, 8, slots)
            picked = picked + jnp.sum(jnp.where(number == target[None], at_z, 0.0), axis=0)
        mean = [picked[c : c + 1] for c in range(3)]
        n = [picked[c : c + 1] for c in range(3, 6)]
        rel = [vel[c, 0] - mean[c] for c in range(3)]
        cross = [n[1] * rel[2] - n[2] * rel[1], n[2] * rel[0] - n[0] * rel[2], n[0] * rel[1] - n[1] * rel[0]]
        along = n[0] * rel[0] + n[1] * rel[1] + n[2] * rel[2]
        turned = [
            mean[c] + cos_angle * rel[c] + sin_angle * cross[c] + (1.0 - cos_angle) * along * n[c]
            for c in range(3)
        ]
        state = columns(stacked([jnp.where(alive > 0, turned[c], vel[c, 0]) for c in range(3)]))
        speed = [state[:, c : c + 1] for c in range(3)]

        lane = iota((slots, slots), 1)
        for step in range(SUBSTEPS):
            speed = [speed[c] + timestep * push[c] / mass_column for c in range(3)]
            place = [place[c] + timestep * speed[c] for c in range(3)]
            block = jnp.zeros((slots, slots), jnp.float32)
            for c, column in enumerate(place):
                block = jnp.where(lane == c, column, block)
            if step == SUBSTEPS - 1:
                for c, column in enumerate(speed):
                    block = jnp.where(lane == 3 + c, column, block)
            flipped = block.T[:8]
            if step < SUBSTEPS - 1:
                sent[step + 1] = jnp.where(comp == 3, alive, flipped)
                copies = exchange(step + 1)
                push = forces(step + 1, copies, place)
        for c in range(3):
            pos_out[c, 0] = jnp.where(alive > 0, flipped[c : c + 1], pos[c, 0])
            vel_out[c, 0] = jnp.where(alive > 0, flipped[3 + c : 4 + c], vel[c, 0])


def rotate_kernel(shape, steps, shift, solvent, occupancy, fields, pos, vel, out, pos_out, vel_out):
    width_x, width_y, width_z = shape
    block_x = width_x // steps
    n_y = width_y // SUB
    rows = 2 * width_y
    step = pl.program_id(0)
    shift_x, shift_y = (shift[0], shift[1])
    double = (iota((rows, width_y), 0) >> 1 == iota((rows, width_y), 1)).astype(jnp.bfloat16)
    row = iota((8, width_z), 0)
    slot = (row & 1).astype(jnp.float32)
    later = ((row >> 1) + shift_y) >= SUB

    @pl.when(step == 0)
    def _():
        pos_out[...] = pos[...]
        vel_out[...] = vel[...]

    def layer(x, carry):
        held = dot(double, occupancy[x].astype(jnp.float32).astype(jnp.bfloat16))
        cell = (step * block_x + x + shift_x) >> 2
        for b in range(n_y):
            at = pl.ds(8 * b, 8)
            both = [
                jnp.where(
                    later, fields[cell, b + 1, pl.ds(c, 1), :], fields[cell, b, pl.ds(c, 1), :]
                )
                for c in range(6)
            ]
            mean, n = (both[:3], both[3:])
            old = [solvent[c, x, at, :] for c in range(3)]
            rel = [old[c] - mean[c] for c in range(3)]
            along = (1.0 - cos_angle) * (n[0] * rel[0] + n[1] * rel[1] + n[2] * rel[2])
            cross = [
                n[1] * rel[2] - n[2] * rel[1],
                n[2] * rel[0] - n[0] * rel[2],
                n[0] * rel[1] - n[1] * rel[0],
            ]
            live = held[8 * b : 8 * b + 8] > slot
            for c in range(3):
                new = mean[c] + cos_angle * rel[c] + sin_angle * cross[c] + along * n[c]
                out[c, x, at, :] = jnp.where(live, new, old[c])
        return carry

    lax.fori_loop(0, block_x, layer, 0)


def per_device(
    solvent_vel,
    occupancy,
    grid_shift,
    axis_index,
    colloid_pos,
    colloid_vel,
    colloid_mass,
    colloid_count,
):
    shape = occupancy.shape
    width_x, width_y, width_z = shape
    rows = 2 * width_y
    n_x, n_y = (width_x // SUB, width_y // SUB)
    slots = colloid_mass.shape[2]
    steps = 4
    block_x = width_x // steps
    solvent = solvent_vel.reshape(3, width_x, rows, width_z)
    smem = pl.BlockSpec(memory_space=pltpu.SMEM)
    vmem = pl.BlockSpec(memory_space=pltpu.VMEM)
    solvent_spec = pl.BlockSpec((3, block_x, rows, width_z), lambda i: (0, i, 0, 0))
    occupancy_spec = pl.BlockSpec((block_x, width_y, width_z), lambda i: (i, 0, 0))
    cells = (n_x + 1, n_y + 1, 8, width_z)
    f32 = jnp.float32

    fields, pos_out, vel_out = pl.pallas_call(
        functools.partial(exchange_kernel, shape, steps),
        grid=(steps,),
        out_shape=[
            jax.ShapeDtypeStruct(cells, f32),
            jax.ShapeDtypeStruct(colloid_pos.shape, f32),
            jax.ShapeDtypeStruct(colloid_vel.shape, f32),
        ],
        in_specs=[smem, smem, solvent_spec, occupancy_spec] + [vmem] * 4,
        out_specs=[vmem] * 3,
        scratch_shapes=[
            pltpu.VMEM((n_x + 1, 3 * rows + width_y, width_z), f32),
            pltpu.VMEM(cells, f32),
            pltpu.VMEM((n_y, 8, width_z), f32),
            pltpu.VMEM((n_x, 8, width_z), f32),
            pltpu.VMEM((8, width_z), f32),
            pltpu.VMEM((n_y, 8, width_z), f32),
            pltpu.VMEM((n_x, 8, width_z), f32),
            pltpu.VMEM((8, width_z), f32),
            pltpu.VMEM((SUBSTEPS, 8, slots), f32),
            pltpu.VMEM((SUBSTEPS, 8, 8, slots), f32),
            pltpu.VMEM((3, slots, slots), f32),
            pltpu.VMEM((3, slots, slots), f32),
            pltpu.SemaphoreType.DMA((6,)),
            pltpu.SemaphoreType.DMA((6,)),
            pltpu.SemaphoreType.DMA((SUBSTEPS, 8)),
            pltpu.SemaphoreType.DMA((SUBSTEPS, 8)),
        ],
        compiler_params=pltpu.CompilerParams(collective_id=0, has_side_effects=True),
        name="exchange",
    )(grid_shift, colloid_count, solvent, occupancy, axis_index, colloid_pos, colloid_vel, colloid_mass)

    turns = 8 if width_x % 8 == 0 else steps
    thin = width_x // turns
    solvent_spec = pl.BlockSpec((3, thin, rows, width_z), lambda i: (0, i, 0, 0))
    occupancy_spec = pl.BlockSpec((thin, width_y, width_z), lambda i: (i, 0, 0))
    solvent_out, pos_out, vel_out = pl.pallas_call(
        functools.partial(rotate_kernel, shape, turns),
        out_shape=[
            jax.ShapeDtypeStruct(solvent.shape, f32),
            jax.ShapeDtypeStruct(colloid_pos.shape, f32),
            jax.ShapeDtypeStruct(colloid_vel.shape, f32),
        ],
        grid=(turns,),
        in_specs=[smem, solvent_spec, occupancy_spec, vmem, vmem, vmem],
        out_specs=[solvent_spec, vmem, vmem],
        name="rotate",
    )(grid_shift, solvent, occupancy, fields, pos_out, vel_out)
    return (solvent_out.reshape(solvent_vel.shape), pos_out, vel_out)


def solution(mesh):
    return jax.shard_map(
        per_device,
        mesh=mesh,
        in_specs=(
            P(None, "gx", "yz", None, None),
            P("gx", "yz", None),
            P(),
            P("gx", "yz", None),
            P(None, "gx", "yz", None),
            P(None, "gx", "yz", None),
            P("gx", "yz", None),
            P("gx", "yz"),
        ),
        out_specs=(
            P(None, "gx", "yz", None, None),
            P(None, "gx", "yz", None),
            P(None, "gx", "yz", None),
        ),
        check_vma=False,
    )
```
